32 devices in a mesh: fsdp: 4 (over y, core), seq: 8 (over z, x).
Axes of the slice: x: 2, y: 2, z: 4, core: 2. Of those that a mesh axis runs over, the one named last changes fastest.
Arguments:
- inputs: bfloat16 [4, 1024, 2560], P('fsdp', 'seq'), may hold values from -6 to 6
- out_grad: bfloat16 [4, 1024, 2560], P('fsdp', 'seq'), may hold values from -6 to 6
- norm_gain: bfloat16 [2560], P(('fsdp', 'seq')), may hold values from 0.5 to 1.5
- w_branch: bfloat16 [2560, 2560], P(('fsdp', 'seq')), may hold values from -0.125 to 0.125
- w_input: bfloat16 [2560, 2560], P(('fsdp', 'seq')), may hold values from -0.125 to 0.125
- conv_weight: bfloat16 [4, 2560], P(None, ('fsdp', 'seq')), may hold values from -3 to 3
- conv_bias: bfloat16 [2560], P(('fsdp', 'seq')), may hold values from -3 to 3
- gate_a_weight: bfloat16 [2560, 256], P(('fsdp', 'seq')), may hold values from -0.375 to 0.375
- gate_a_bias: bfloat16 [2560], P(('fsdp', 'seq')), may hold values from -4 to 4
- gate_x_weight: bfloat16 [2560, 256], P(('fsdp', 'seq')), may hold values from -0.375 to 0.375
- gate_x_bias: bfloat16 [2560], P(('fsdp', 'seq')), may hold values from -4 to 4
- lru_param: bfloat16 [2560], P(('fsdp', 'seq')), may hold values from -14 to -3, as said below
- w_out: bfloat16 [2560, 2560], P(('fsdp', 'seq')), may hold values from -0.25 to 0.25
- mlp_norm_gain: bfloat16 [2560], P(('fsdp', 'seq')), may hold values from 0.5 to 1.5
- w_gate_up: bfloat16 [2560, 2, 7680], P(None, None, ('fsdp', 'seq')), may hold values from -0.125 to 0.125
- w_down: bfloat16 [7680, 2560], P(('fsdp', 'seq')), may hold values from -0.09375 to 0.09375
Outputs:
- outputs: bfloat16 [4, 1024, 2560], P('fsdp', 'seq')
- input_grad: bfloat16 [4, 1024, 2560], P('fsdp', 'seq')
- grad_norm_gain: float32 [2560], P(('fsdp', 'seq'))
- grad_w_branch: float32 [2560, 2560], P(('fsdp', 'seq'))
- grad_w_input: float32 [2560, 2560], P(('fsdp', 'seq'))
- grad_conv_weight: float32 [4, 2560], P(None, ('fsdp', 'seq'))
- grad_conv_bias: float32 [2560], P(('fsdp', 'seq'))
- grad_gate_a_weight: float32 [2560, 256], P(('fsdp', 'seq'))
- grad_gate_a_bias: float32 [2560], P(('fsdp', 'seq'))
- grad_gate_x_weight: float32 [2560, 256], P(('fsdp', 'seq'))
- grad_gate_x_bias: float32 [2560], P(('fsdp', 'seq'))
- grad_lru_param: float32 [2560], P(('fsdp', 'seq'))
- grad_w_out: float32 [2560, 2560], P(('fsdp', 'seq'))
- grad_mlp_norm_gain: float32 [2560], P(('fsdp', 'seq'))
- grad_w_gate_up: float32 [2560, 2, 7680], P(None, None, ('fsdp', 'seq'))
- grad_w_down: float32 [7680, 2560], P(('fsdp', 'seq'))
The draws below stay inside these ranges and needn't reach their ends.
Inputs may be any that keep to these rules, and one draw needn't show every extreme that they name: `lru_param`: one value for each channel, drawn independently.
All inputs are finite; a program needn't handle non-finite values.
Results may differ from the reference program's by a relative error of at most 0.015.
Values may be sent and summed in bfloat16 or wider, within the bound.
A program may use at most 576 MiB of HBM per device.

```python
import math
import jax
import jax.numpy as jnp
from jax import lax

D = 2560
FF = 7680
HEAD = 256
LENGTH = 1024
SEQUENCES = 4


def draw_lru_param(key, part):
    key_kind, key_total, key_span = jax.random.split(jax.random.fold_in(key, 7), 3)
    slow_share = 0.5
    is_slow = jax.random.bernoulli(key_kind, slow_share, (D,))
    total_loss = jnp.exp(jax.random.uniform(key_total, (D,), jnp.float32, math.log(0.3), math.log(1.5)))
    forget_span = jnp.exp(jax.random.uniform(key_span, (D,), jnp.float32, math.log(30.0), math.log(50.0)))
    rates = jnp.where(is_slow, total_loss / (4.0 * LENGTH), 2.3 / (4.0 * forget_span))
    return jnp.log(jnp.expm1(rates)).astype(jnp.bfloat16)


def raised(array, stream_key, source, target, parts, factor):
    owner, partner = [(jnp.arange(array.shape[dim]) // (array.shape[dim] // parts)).reshape([-1 if axis == dim else 1 for axis in range(array.ndim)]) for dim in (source, target)]
    chosen = jax.random.permutation(stream_key, parts)[partner]
    strong = (owner == chosen) | (owner == (partner + parts // 2) % parts)
    return jnp.where(strong, factor * array, array)


def level_of(stream_key, extent, pieces, smallest, largest):
    loudness, own = 1.0, jax.random.fold_in(stream_key, 6)
    for position, blocks in pieces:
        heights = jnp.exp(jax.random.uniform(jax.random.fold_in(own, position), (blocks,), jnp.float32, smallest / len(pieces), largest / len(pieces)))
        loudness = loudness * jnp.repeat(heights, extent[position] // blocks).reshape([-1 if axis == position else 1 for axis in range(len(extent))])
    return loudness


def centred(stream_key, shape, width, most, cuts=(), held_as=jnp.bfloat16):
    entries = width * jax.random.normal(stream_key, shape, jnp.float32)
    if cuts:
        entries = entries * level_of(stream_key, shape, cuts, -0.22, 0.18)
    return jnp.clip(entries, -most, most).astype(held_as)


def bell_draw_with(key, shape, spread, most, cuts, heavy, kind=jnp.bfloat16):
    drawn = spread * jax.random.normal(key, shape, jnp.float32)
    if cuts:
        drawn = drawn * level_of(key, shape, cuts, -0.22, 0.18)
    return jnp.clip(raised(drawn, jax.random.fold_in(key, 3), *heavy), -most, most).astype(kind)


def setup_inputs(seed: int = 0) -> dict:
    seeds = jax.random.split(jax.random.key(seed), 17)
    inputs = bell_draw_with(seeds[0], (SEQUENCES, LENGTH, D), 1.0, 6.0, ((0, 4), (1, 8)), (1, 2, 8, 2.0))
    out_grad = centred(seeds[1], (SEQUENCES, LENGTH, D), 1.0, 6.0, ((0, 4), (1, 8)))
    norm_gain = jnp.clip(1.0 + 0.1 * jax.random.normal(seeds[2], (D,), jnp.float32), 0.5, 1.5).astype(jnp.bfloat16)
    w_branch = centred(seeds[3], (D, D), D ** -0.5, 0.125, ((0, 32),))
    w_input = centred(seeds[4], (D, D), D ** -0.5, 0.125, ((0, 32),))
    conv_weight = centred(seeds[5], (4, D), 0.5, 3.0, ((1, 32),))
    conv_bias = centred(seeds[6], (D,), 0.5, 3.0, ((0, 32),))
    gate_a_weight = centred(seeds[7], (D, HEAD), HEAD ** -0.5, 0.375, ((0, 32),))
    gate_a_bias = centred(seeds[8], (D,), 1.0, 4.0, ((0, 32),))
    gate_x_weight = centred(seeds[9], (D, HEAD), HEAD ** -0.5, 0.375, ((0, 32),))
    gate_x_bias = centred(seeds[10], (D,), 1.0, 4.0, ((0, 32),))
    lru_param = draw_lru_param(jax.random.fold_in(seeds[16], 71), 0)
    w_out = centred(seeds[12], (D, D), (D // 4) ** -0.5, 0.25, ((0, 32),))
    mlp_norm_gain = jnp.clip(1.0 + 0.1 * jax.random.normal(seeds[13], (D,), jnp.float32), 0.5, 1.5).astype(jnp.bfloat16)
    w_gate_up = centred(seeds[14], (D, 2, FF), D ** -0.5, 0.125, ((2, 32),))
    w_down = centred(seeds[15], (FF, D), (FF // 2) ** -0.5, 0.09375, ((0, 32),))
    return dict(inputs=inputs, out_grad=out_grad, norm_gain=norm_gain, w_branch=w_branch, w_input=w_input, conv_weight=conv_weight, conv_bias=conv_bias, gate_a_weight=gate_a_weight, gate_a_bias=gate_a_bias, gate_x_weight=gate_x_weight, gate_x_bias=gate_x_bias, lru_param=lru_param, w_out=w_out, mlp_norm_gain=mlp_norm_gain, w_gate_up=w_gate_up, w_down=w_down)


EPS = 1e-06

def to_bf16(values):
    return lax.optimization_barrier(values.astype(jnp.bfloat16))

def gelu_tanh(values):
    return jax.nn.gelu(values, approximate=True)

def block_forward(values, weight, head_count):
    length, model_width = values.shape
    head_size = weight.shape[1]
    result = jnp.einsum('lhm,hmi->lhi', values.astype(jnp.float32).reshape(length, head_count, head_size), weight.astype(jnp.float32).reshape(head_count, head_size, head_size))
    return result.reshape(length, model_width)

def block_backward(grads_in, weight, head_count):
    length, model_width = grads_in.shape
    head_size = weight.shape[1]
    result = jnp.einsum('lhi,hmi->lhm', grads_in.astype(jnp.float32).reshape(length, head_count, head_size), weight.astype(jnp.float32).reshape(head_count, head_size, head_size))
    return result.reshape(length, model_width)

def block_weight_grad(values, grads_in, head_count):
    length, model_width = values.shape
    head_size = model_width // head_count
    result = jnp.einsum('lhm,lhi->hmi', values.astype(jnp.float32).reshape(length, head_count, head_size), grads_in.astype(jnp.float32).reshape(length, head_count, head_size))
    return result.reshape(model_width, head_size)

def recurrence(log_f, gated_f):
    length = log_f.shape[0]
    is_first = (jnp.arange(length) == 0)[:, None]
    decays = jnp.exp(log_f)
    norm_mult = jnp.where(is_first, 1.0, jnp.sqrt(-jnp.expm1(2.0 * log_f)))
    drives = norm_mult * gated_f

    def advance(states, step_in):
        decay_now, drive_now = step_in
        states = decay_now * states + drive_now
        return (states, states)
    _, result = lax.scan(advance, jnp.zeros(log_f.shape[1], log_f.dtype), (decays, drives))
    return result

def reference(inputs, out_grad, norm_gain, w_branch, w_input, conv_weight, conv_bias, gate_a_weight, gate_a_bias, gate_x_weight, gate_x_bias, lru_param, w_out, mlp_norm_gain, w_gate_up, w_down):
    model_width = inputs.shape[2]
    hidden_width = w_down.shape[0]
    head_count = model_width // gate_a_weight.shape[1]
    gain_f = norm_gain.astype(jnp.float32)
    gain_two = mlp_norm_gain.astype(jnp.float32)
    conv_w = conv_weight.astype(jnp.float32)
    conv_b = conv_bias.astype(jnp.float32)
    bias_a = gate_a_bias.astype(jnp.float32)
    bias_x = gate_x_bias.astype(jnp.float32)
    lru_f = lru_param.astype(jnp.float32)
    soft_rate = jax.nn.softplus(lru_f)
    lru_slope = jax.nn.sigmoid(lru_f)
    gate_up_flat = w_gate_up.reshape(model_width, 2 * hidden_width)

    def one_sequence(running, pair_in):
        seq_in, seq_cot = pair_in
        length = seq_in.shape[0]
        flat_in = seq_in.astype(jnp.float32)
        inv_rms = lax.rsqrt(lax.optimization_barrier(jnp.mean(flat_in * flat_in, axis=1, keepdims=True)) + EPS)
        scaled = flat_in * inv_rms
        normed = to_bf16(scaled * gain_f)
        branch_pre = jnp.dot(normed, w_branch, preferred_element_type=jnp.float32)
        input_pre = to_bf16(jnp.dot(normed, w_input, preferred_element_type=jnp.float32))
        extended = jnp.concatenate([jnp.zeros((3, model_width), jnp.float32), input_pre.astype(jnp.float32)], axis=0)
        conv_out = conv_b + jnp.zeros((length, model_width), jnp.float32)
        for tap_index in range(4):
            conv_out = conv_out + conv_w[tap_index] * extended[3 - tap_index:3 - tap_index + length]
        conv_in = to_bf16(conv_out)
        rate_gate = jax.nn.sigmoid(block_forward(conv_in, gate_a_weight, head_count) + bias_a)
        input_gate = jax.nn.sigmoid(block_forward(conv_in, gate_x_weight, head_count) + bias_x)
        log_a = to_bf16(-8.0 * rate_gate * soft_rate)
        gated_in = to_bf16(input_gate * conv_out)
        states, lru_back = jax.vjp(recurrence, log_a.astype(jnp.float32), gated_in.astype(jnp.float32))
        hidden = to_bf16(states)
        branch_act, gelu_back = jax.vjp(gelu_tanh, branch_pre)
        mixed_rows = to_bf16(hidden.astype(jnp.float32) * branch_act)
        mid = flat_in + jnp.dot(mixed_rows, w_out, preferred_element_type=jnp.float32)
        inv_two = lax.rsqrt(lax.optimization_barrier(jnp.mean(mid * mid, axis=1, keepdims=True)) + EPS)
        scaled_two = mid * inv_two
        normed_two = to_bf16(scaled_two * gain_two)
        gate_up = jnp.dot(normed_two, gate_up_flat, preferred_element_type=jnp.float32)
        gate_pre = gate_up[:, :hidden_width]
        up_pre = gate_up[:, hidden_width:]
        gelu_val, gelu_two_back = jax.vjp(gelu_tanh, gate_pre)
        mlp_hidden = to_bf16(gelu_val * up_pre)
        seq_out = to_bf16(mid + jnp.dot(mlp_hidden, w_down, preferred_element_type=jnp.float32))
        grad_down_term = jnp.dot(mlp_hidden.T, seq_cot, preferred_element_type=jnp.float32)
        d_mlp_hidden = jnp.dot(seq_cot, w_down.T, preferred_element_type=jnp.float32)
        d_gate_up = to_bf16(jnp.concatenate([gelu_two_back(d_mlp_hidden * up_pre)[0], d_mlp_hidden * gelu_val], axis=1))
        grad_gate_up_term = jnp.dot(normed_two.T, d_gate_up, preferred_element_type=jnp.float32).reshape(model_width, 2, hidden_width)
        d_normed_two = jnp.dot(d_gate_up, gate_up_flat.T, preferred_element_type=jnp.float32)
        d_scaled_two = d_normed_two * gain_two
        d_mid = seq_cot.astype(jnp.float32) + inv_two * (d_scaled_two - scaled_two * lax.optimization_barrier(jnp.mean(d_scaled_two * scaled_two, axis=1, keepdims=True)))
        mid_cot = to_bf16(d_mid)
        grad_out_term = jnp.dot(mixed_rows.T, mid_cot, preferred_element_type=jnp.float32)
        d_mixed = jnp.dot(mid_cot, w_out.T, preferred_element_type=jnp.float32)
        d_hidden = to_bf16(d_mixed * branch_act)
        d_branch_pre = to_bf16(gelu_back(d_mixed * hidden.astype(jnp.float32))[0])
        d_log_f, d_gated_f = lru_back(d_hidden.astype(jnp.float32))
        d_log = to_bf16(d_log_f).astype(jnp.float32)
        d_gated = to_bf16(d_gated_f).astype(jnp.float32)
        d_rate_pre_f = d_log * (-8.0 * soft_rate) * rate_gate * (1.0 - rate_gate)
        d_gate_pre_f = d_gated * conv_out * input_gate * (1.0 - input_gate)
        d_rate_pre = to_bf16(d_rate_pre_f)
        d_gate_pre = to_bf16(d_gate_pre_f)
        d_conv = d_gated * input_gate + block_backward(d_rate_pre, gate_a_weight, head_count) + block_backward(d_gate_pre, gate_x_weight, head_count)
        ext_back = jnp.concatenate([d_conv, jnp.zeros((3, model_width), jnp.float32)], axis=0)
        d_input = jnp.zeros((length, model_width), jnp.float32)
        for tap_index in range(4):
            d_input = d_input + conv_w[tap_index] * ext_back[tap_index:tap_index + length]
        d_input_pre = to_bf16(d_input)
        d_normed = jnp.dot(d_branch_pre, w_branch.T, preferred_element_type=jnp.float32) + jnp.dot(d_input_pre, w_input.T, preferred_element_type=jnp.float32)
        d_scaled = d_normed * gain_f
        seq_dx = to_bf16(d_mid + inv_rms * (d_scaled - scaled * lax.optimization_barrier(jnp.mean(d_scaled * scaled, axis=1, keepdims=True))))
        conv_terms = jnp.stack([lax.optimization_barrier(jnp.sum(extended[3 - tap_index:3 - tap_index + length] * d_conv, axis=0)) for tap_index in range(4)])
        terms = (lax.optimization_barrier(jnp.sum(scaled * d_normed, axis=0)), jnp.dot(normed.T, d_branch_pre, preferred_element_type=jnp.float32), jnp.dot(normed.T, d_input_pre, preferred_element_type=jnp.float32), conv_terms, lax.optimization_barrier(jnp.sum(d_conv, axis=0)), block_weight_grad(conv_in, d_rate_pre, head_count), lax.optimization_barrier(jnp.sum(d_rate_pre_f, axis=0)), block_weight_grad(conv_in, d_gate_pre, head_count), lax.optimization_barrier(jnp.sum(d_gate_pre_f, axis=0)), lax.optimization_barrier(jnp.sum(d_log * (-8.0 * rate_gate), axis=0)) * lru_slope, grad_out_term, lax.optimization_barrier(jnp.sum(scaled_two * d_normed_two, axis=0)), grad_gate_up_term, grad_down_term)
        running = jax.tree.map(lambda summed, adding: summed + adding, running, terms)
        return (running, (seq_out, seq_dx))
    head_size = gate_a_weight.shape[1]
    zero_grads = (jnp.zeros((model_width,), jnp.float32), jnp.zeros((model_width, model_width), jnp.float32), jnp.zeros((model_width, model_width), jnp.float32), jnp.zeros((4, model_width), jnp.float32), jnp.zeros((model_width,), jnp.float32), jnp.zeros((model_width, head_size), jnp.float32), jnp.zeros((model_width,), jnp.float32), jnp.zeros((model_width, head_size), jnp.float32), jnp.zeros((model_width,), jnp.float32), jnp.zeros((model_width,), jnp.float32), jnp.zeros((model_width, model_width), jnp.float32), jnp.zeros((model_width,), jnp.float32), jnp.zeros((model_width, 2, hidden_width), jnp.float32), jnp.zeros((hidden_width, model_width), jnp.float32))
    grad_sums, (outputs, input_grad) = lax.scan(one_sequence, zero_grads, (inputs, out_grad))
    return (outputs, input_grad, grad_sums[0], grad_sums[1], grad_sums[2], grad_sums[3], grad_sums[4], grad_sums[5], grad_sums[6], grad_sums[7], grad_sums[8], grad_sums[9], grad_sums[10], grad_sums[11], grad_sums[12], grad_sums[13])
```

```python
import jax
import jax.numpy as jnp
from jax import lax
from jax.experimental import pallas as pl
from jax.experimental.pallas import tpu as pltpu
from jax.sharding import PartitionSpec as P

EPS = 1e-06
CORES = 2
XDIM = 2
BOTH = ("fsdp", "seq")
F32 = jnp.float32
BF16 = jnp.bfloat16


def rounded(values):
    return values.astype(BF16)


def gelu_tanh(values):
    return jax.nn.gelu(values, approximate=True)


def dot(left, right):
    return jnp.dot(left, right, preferred_element_type=F32)


def dot_t(left, right):
    return lax.dot_general(left, right, (((1,), (1,)), ((), ())), preferred_element_type=F32)


def contract_rows(left, right):
    return lax.dot_general(left, right, (((0,), (0,)), ((), ())), preferred_element_type=F32)


class Place:
    def __init__(self):
        self.nf, self.ns = lax.axis_size("fsdp"), lax.axis_size("seq")
        self.ny, self.nc = self.nf // CORES, CORES
        self.nz, self.nx = self.ns // XDIM, XDIM
        f, s = lax.axis_index("fsdp"), lax.axis_index("seq")
        self.y, self.c, self.z, self.x, self.s = f // CORES, f % CORES, s // XDIM, s % XDIM, s

    def shift(self, value, dy=0, dc=0, dz=0, dx=0):
        pairs = []
        for source in range(self.nf * self.ns):
            f, s = divmod(source, self.ns)
            y, c = divmod(f, self.nc)
            z, x = divmod(s, self.nx)
            y, c = (y + dy) % self.ny, (c + dc) % self.nc
            z, x = (z + dz) % self.nz, (x + dx) % self.nx
            pairs.append((source, (y * self.nc + c) * self.ns + z * self.nx + x))
        return lax.ppermute(value, BOTH, pairs)

    def along_seq(self, value, steps):
        first, last = max(0, -steps), min(self.ns, self.ns - steps)
        return lax.ppermute(value, "seq", [(i, i + steps) for i in range(first, last)])


def gather_tokens(at, value):
    line = [value]
    for _ in range(1, at.nz):
        line.append(at.shift(line[-1], dz=1))
    return [[v] + [at.shift(v, dy=j) for j in range(1, at.ny)] for v in line]


def scatter_tokens(at, parts):
    total = None
    for k in range(at.nz):
        here = parts[k][0]
        for j in range(1, at.ny):
            here = here + at.shift(rounded(parts[k][j]), dy=-j).astype(F32)
        if k:
            here = at.shift(rounded(here), dz=-k).astype(F32)
        total = here if total is None else total + here
    return total


def gather_shards(at, value, place):
    line = [value]
    for _ in range(1, at.nz):
        line.append(at.shift(line[-1], dz=1))
    buffer = None
    for k, v in enumerate(line):
        for i in range(at.nx):
            w = at.shift(v, dx=i) if i else v
            for h in range(at.nc):
                u = at.shift(w, dc=h) if h else w
                buffer = place(buffer, u, (at.c - h) % at.nc, (at.z - k) % at.nz, (at.x - i) % at.nx)
    return buffer


def take(values, index):
    return lax.dynamic_index_in_dim(values, index, 0, keepdims=False)


def scatter_shards(at, values, kind=BF16):
    mine = take(values, at.c).astype(F32)
    for h in range(1, at.nc):
        mine = mine + at.shift(take(values, (at.c - h) % at.nc).astype(kind), dc=-h).astype(F32)
    mine = jnp.swapaxes(mine, 0, 1)
    here = take(mine, at.x)
    for i in range(1, at.nx):
        here = here + at.shift(take(mine, (at.x - i) % at.nx).astype(kind), dx=-i).astype(F32)
    total = take(here, at.z)
    for k in range(1, at.nz):
        total = total + at.shift(take(here, (at.z - k) % at.nz).astype(kind), dz=-k).astype(F32)
    return total


def scan_steps(coeff, value, reverse):
    count = coeff.shape[0]
    rows = lax.broadcasted_iota(jnp.int32, coeff.shape, 0)
    step = 1
    while step < count:
        if reverse:
            inside = rows < count - step
            moved = count - step
        else:
            inside = rows >= step
            moved = step
        value = value + coeff * jnp.where(inside, pltpu.roll(value, moved, 0), 0.0)
        coeff = coeff * jnp.where(inside, pltpu.roll(coeff, moved, 0), 1.0)
        step *= 2
    return coeff, value


def forward_scan_kernel(decay_ref, drive_ref, prod_ref, state_ref):
    prod_ref[...], state_ref[...] = scan_steps(decay_ref[...], drive_ref[...], False)


def backward_scan_kernel(decay_ref, grad_ref, prod_ref, state_ref):
    decays = decay_ref[...]
    count = decays.shape[0]
    rows = lax.broadcasted_iota(jnp.int32, decays.shape, 0)
    following = jnp.where(rows < count - 1, pltpu.roll(decays, count - 1, 0), 1.0)
    prod_ref[...], state_ref[...] = scan_steps(following, grad_ref[...], True)


def local_scan(kernel, decays, drives):
    groups, count, width = decays.shape
    tile = 256 if width % 256 == 0 else width
    spec = pl.BlockSpec((None, count, tile), lambda g, t: (g, 0, t))
    shape = jax.ShapeDtypeStruct(decays.shape, F32)
    return pl.pallas_call(
        kernel,
        grid=(groups, width // tile),
        in_specs=[spec, spec],
        out_specs=[spec, spec],
        out_shape=[shape, shape],
        cost_estimate=pl.CostEstimate(
            flops=40 * decays.size, bytes_accessed=16 * decays.size, transcendentals=0
        ),
    )(decays, drives)


def carried(at, prod, last, sign):
    both = jnp.stack([prod, last])
    pieces = [at.along_seq(both, sign * k) for k in range(1, at.ns)]
    carry = jnp.zeros_like(last)
    for piece in reversed(pieces):
        carry = piece[1] + piece[0] * carry
    return carry


def body(
    inputs,
    out_grad,
    norm_gain,
    w_branch,
    w_input,
    conv_weight,
    conv_bias,
    gate_a_weight,
    gate_a_bias,
    gate_x_weight,
    gate_x_bias,
    lru_param,
    w_out,
    mlp_norm_gain,
    w_gate_up,
    w_down,
):
    at = Place()
    rows, width = inputs.shape[0] * inputs.shape[1], inputs.shape[2]
    shard = w_branch.shape[0]
    head = gate_a_weight.shape[1]
    half = width // at.ny
    taps = conv_weight.shape[0]
    hid = w_down.shape[0]
    local_in = inputs.reshape(rows, width)
    cot = out_grad.reshape(rows, width)

    vectors = jnp.concatenate(
        [conv_weight, jnp.stack([conv_bias, gate_a_bias, gate_x_bias, lru_param, norm_gain, mlp_norm_gain])]
    )
    nvec = taps + 6
    vectors = jnp.pad(vectors, ((0, -nvec % 16), (0, head - shard)))
    small = jnp.concatenate([gate_a_weight, gate_x_weight, vectors], axis=0)
    small = lax.all_gather(small, BOTH, axis=0, tiled=False)
    small_y = lax.dynamic_slice_in_dim(small, at.y * (at.nf // at.ny) * at.ns, small.shape[0] // at.ny, 0)
    gate_a = small_y[:, :shard, :].reshape(half, head)
    gate_x = small_y[:, shard : 2 * shard, :].reshape(half, head)

    def vector(index, source):
        return source[:, 2 * shard + index, :shard].reshape(-1).astype(F32)

    conv_w = jnp.stack([vector(i, small_y) for i in range(taps)])
    conv_b, bias_a, bias_x, lru_f = [vector(taps + i, small_y) for i in range(4)]
    gain = vector(taps + 4, small)
    gain_two = vector(taps + 5, small)

    own_in = [local_in] + [at.shift(local_in, dy=j) for j in range(1, at.ny)]
    group_in = jnp.concatenate(own_in, axis=0)

    def half_columns(weight, j):
        return lax.dynamic_slice_in_dim(weight, ((at.y + j) % at.ny) * half, half, 1)

    piece = jnp.zeros((at.ny, shard, 2 * half), BF16)
    for j in range(at.ny):
        part = jnp.concatenate([half_columns(w_branch, j), half_columns(w_input, j)], axis=1)
        part = at.shift(part, dy=j) if j else part
        piece = lax.dynamic_update_index_in_dim(piece, part, (at.y - j) % at.ny, 0)

    def place_in(buffer, value, c, z, x):
        if buffer is None:
            buffer = jnp.zeros((at.ny, at.nc, at.nz, at.nx, shard, 2 * half), BF16)
        return lax.dynamic_update_slice(buffer, value[:, None, None, None], (0, c, z, x, 0, 0))

    def place_out(buffer, value, c, z, x):
        if buffer is None:
            buffer = jnp.zeros((at.nc, at.nz, at.nx, shard, width), BF16)
        return lax.dynamic_update_slice(buffer, value[None, None, None], (c, z, x, 0, 0))

    w_two = gather_shards(at, piece, place_in).reshape(width, 2 * half)
    w_out_half = gather_shards(at, w_out, place_out).reshape(half, width)

    w_pack = jnp.concatenate([jnp.transpose(w_gate_up, (1, 2, 0)), w_down[None]], axis=0)
    slots = []
    for i in range(at.nx):
        v = at.shift(w_pack, dx=i) if i else w_pack
        slots += [at.shift(v, dc=h) if h else v for h in range(at.nc)]
    nslot = len(slots)
    w_all = jnp.stack(slots, axis=1).reshape(3, nslot * hid, width)
    w_gate, w_up, w_dn = w_all[0], w_all[1], w_all[2]

    cot_slots = gather_tokens(at, cot)

    group_f = group_in.astype(F32)
    inv_rms = lax.rsqrt(jnp.mean(group_f * group_f, axis=1, keepdims=True) + EPS)
    normed = rounded(group_f * inv_rms * gain)
    pre = dot(normed, w_two)
    branch_pre = pre[:, :half]
    input_pre = rounded(pre[:, half:]).reshape(at.ny, rows, half)
    edge_prev = at.along_seq(input_pre[:, rows - taps + 1 :, :], 1)
    extended = jnp.concatenate([edge_prev, input_pre], axis=1).astype(F32)
    conv_out = conv_b
    for tap in range(taps):
        conv_out = conv_out + conv_w[tap] * extended[:, taps - 1 - tap : taps - 1 - tap + rows, :]
    conv_rows = conv_out.reshape(at.ny * rows, half)
    conv_in = rounded(conv_rows)

    heads = half // head
    same = (jnp.arange(half) // head)[:, None] == (jnp.arange(half) // head)[None, :]

    def dense(weight):
        return jnp.where(same, jnp.tile(weight, (1, heads)), jnp.zeros((), BF16))

    dense_a, dense_x = dense(gate_a), dense(gate_x)
    rate_gate = jax.nn.sigmoid(dot(conv_in, dense_a) + bias_a)
    input_gate = jax.nn.sigmoid(dot(conv_in, dense_x) + bias_x)
    soft_rate = jax.nn.softplus(lru_f)
    log_a = rounded(-8.0 * rate_gate * soft_rate)
    gated_in = rounded(input_gate * conv_rows)
    log_f = log_a.astype(F32).reshape(at.ny, rows, half)
    gated_f = gated_in.astype(F32).reshape(at.ny, rows, half)
    is_first = (lax.broadcasted_iota(jnp.int32, log_f.shape, 1) == 0) & (at.s == 0)
    decays = jnp.exp(log_f)
    norm_mult = jnp.where(is_first, 1.0, jnp.sqrt(-jnp.expm1(2.0 * log_f)))
    prods, local_states = local_scan(forward_scan_kernel, decays, norm_mult * gated_f)
    block_prod = prods[:, rows - 1, :]
    state_in = carried(at, block_prod, local_states[:, rows - 1, :], 1)
    states = local_states + prods * state_in[:, None, :]
    hidden = rounded(states)
    hidden_rows = hidden.reshape(at.ny * rows, half).astype(F32)
    branch_act, gelu_back = jax.vjp(gelu_tanh, branch_pre)
    mixed = rounded(hidden_rows * branch_act)
    mixed_out = dot(mixed, w_out_half).reshape(at.ny, rows, width)
    mid = local_in.astype(F32) + mixed_out[0]
    for j in range(1, at.ny):
        mid = mid + at.shift(rounded(mixed_out[j]), dy=-j).astype(F32)

    inv_two = lax.rsqrt(jnp.mean(mid * mid, axis=1, keepdims=True) + EPS)
    scaled_two = mid * inv_two
    normed_two = rounded(scaled_two * gain_two)
    token_slots = gather_tokens(at, normed_two)
    out_parts, back_parts = [], []
    saved = []
    for k in range(at.nz):
        tokens = jnp.concatenate(token_slots[k], axis=0)
        cots = jnp.concatenate(cot_slots[k], axis=0)
        gate_pre = dot_t(tokens, w_gate)
        up_pre = dot_t(tokens, w_up)
        d_hid = dot_t(cots, w_dn)
        gelu_val, gelu_two_back = jax.vjp(gelu_tanh, gate_pre)
        mlp_hidden = rounded(gelu_val * up_pre)
        d_gate = rounded(gelu_two_back(d_hid * up_pre)[0])
        d_up = rounded(d_hid * gelu_val)
        back = dot(d_gate, w_gate) + dot(d_up, w_up)
        out = dot(mlp_hidden, w_dn)
        back_parts.append(list(back.reshape(at.ny, rows, width)))
        out_parts.append(list(out.reshape(at.ny, rows, width)))
        saved.append((tokens, cots, mlp_hidden, d_gate, d_up))
    d_normed_two = scatter_tokens(at, back_parts)
    outputs = rounded(mid + scatter_tokens(at, out_parts)).reshape(inputs.shape)
    tokens, cots, mlp_hidden, d_gate, d_up = [jnp.concatenate(v, axis=0) for v in zip(*saved)]
    d_w = jnp.stack(
        [
            rounded(contract_rows(d_gate, tokens)),
            rounded(contract_rows(d_up, tokens)),
            rounded(contract_rows(mlp_hidden, cots)),
        ]
    ).reshape(3, at.nx, at.nc, hid, width)
    mine = d_w[:, :, 0].astype(F32)
    for h in range(1, at.nc):
        mine = mine + at.shift(d_w[:, :, h], dc=-h).astype(F32)
    total = mine[:, 0]
    for i in range(1, at.nx):
        total = total + at.shift(rounded(mine[:, i]), dx=-i).astype(F32)
    grad_w_gate_up = jnp.transpose(total[:2], (2, 0, 1))
    grad_w_down = total[2]

    grad_gain_two = jnp.sum(scaled_two * d_normed_two, axis=0)
    d_scaled_two = d_normed_two * gain_two
    d_mid = cot.astype(F32) + inv_two * (
        d_scaled_two - scaled_two * jnp.mean(d_scaled_two * scaled_two, axis=1, keepdims=True)
    )
    mid_cot = rounded(d_mid)

    group_cot = jnp.concatenate([mid_cot] + [at.shift(mid_cot, dy=j) for j in range(1, at.ny)], axis=0)
    d_mixed = dot_t(group_cot, w_out_half)
    shards = (at.nc, at.nz, at.nx)
    grad_out_part = rounded(contract_rows(mixed, group_cot)).reshape(*shards, shard, width)
    grad_w_out = scatter_shards(at, grad_out_part)
    d_hidden = rounded(d_mixed * branch_act).astype(F32).reshape(at.ny, rows, half)
    d_branch_pre = rounded(gelu_back(d_mixed * hidden_rows)[0])
    back_prods, local_grads = local_scan(backward_scan_kernel, decays, d_hidden)
    grad_in = carried(at, block_prod, decays[:, 0, :] * local_grads[:, 0, :], -1)
    grad_states = local_grads + back_prods * grad_in[:, None, :]
    state_prev = jnp.concatenate([state_in[:, None, :], states[:, : rows - 1, :]], axis=1)
    d_log = rounded(
        decays * grad_states * state_prev
        - jnp.where(is_first, 0.0, grad_states * gated_f * decays * decays / norm_mult)
    )
    d_gated = rounded(grad_states * norm_mult)
    d_log = d_log.astype(F32).reshape(at.ny * rows, half)
    d_gated = d_gated.astype(F32).reshape(at.ny * rows, half)
    d_rate_pre_f = d_log * (-8.0 * soft_rate) * rate_gate * (1.0 - rate_gate)
    d_gate_pre_f = d_gated * conv_rows * input_gate * (1.0 - input_gate)
    d_rate_pre = rounded(d_rate_pre_f)
    d_gate_pre = rounded(d_gate_pre_f)
    grad_lru = jnp.sum(d_log * (-8.0 * rate_gate), axis=0) * jax.nn.sigmoid(lru_f)
    grad_bias_a = jnp.sum(d_rate_pre_f, axis=0)
    grad_bias_x = jnp.sum(d_gate_pre_f, axis=0)
    d_conv = d_gated * input_gate + dot_t(d_rate_pre, dense_a) + dot_t(d_gate_pre, dense_x)
    d_conv_blocks = d_conv.reshape(at.ny, rows, half)
    edge_next = at.along_seq(d_conv_blocks[:, : taps - 1, :], -1)
    ext_back = jnp.concatenate([d_conv_blocks, edge_next], axis=1)
    d_input = conv_w[0] * d_conv_blocks
    for tap in range(1, taps):
        d_input = d_input + conv_w[tap] * ext_back[:, tap : tap + rows, :]
    d_input_pre = rounded(d_input.reshape(at.ny * rows, half))
    d_normed_part = dot_t(jnp.concatenate([d_branch_pre, d_input_pre], axis=1), w_two)
    d_normed_part = d_normed_part.reshape(at.ny, rows, width)
    d_normed = d_normed_part[0]
    for j in range(1, at.ny):
        d_normed = d_normed + at.shift(rounded(d_normed_part[j]), dy=-j).astype(F32)
    inv_own = inv_rms[:rows]
    scaled = local_in.astype(F32) * inv_own
    grad_gain = jnp.sum(scaled * d_normed, axis=0)
    d_scaled = d_normed * gain
    input_grad = rounded(
        d_mid + inv_own * (d_scaled - scaled * jnp.mean(d_scaled * scaled, axis=1, keepdims=True))
    ).reshape(inputs.shape)

    def column_grad(part):
        parts = rounded(contract_rows(normed, part)).reshape(at.ny, *shards, shard, half)
        got = scatter_shards(at, jnp.moveaxis(parts, 0, 3))
        own = take(got, at.y)
        whole = jnp.zeros((shard, at.ny, half), F32)
        whole = lax.dynamic_update_slice(whole, own[:, None, :], (0, at.y, 0))
        for j in range(1, at.ny):
            other = at.shift(rounded(take(got, (at.y - j) % at.ny)), dy=-j).astype(F32)
            whole = lax.dynamic_update_slice(whole, other[:, None, :], (0, (at.y + j) % at.ny, 0))
        return whole.reshape(shard, width)

    grad_branch = column_grad(d_branch_pre)
    grad_input = column_grad(d_input_pre)

    def diagonal(full):
        return jnp.concatenate(
            [full[h * head : (h + 1) * head, h * head : (h + 1) * head] for h in range(heads)], axis=0
        )

    grad_gates = jnp.concatenate(
        [diagonal(contract_rows(conv_in, d_rate_pre)), diagonal(contract_rows(conv_in, d_gate_pre))], axis=1
    )
    grad_gates = scatter_shards(at, grad_gates.reshape(*shards, shard, 2 * head), F32)
    grad_gate_a, grad_gate_x = grad_gates[:, :head], grad_gates[:, head:]

    conv_sums = [
        jnp.sum(extended[:, taps - 1 - tap : taps - 1 - tap + rows, :] * d_conv_blocks, axis=(0, 1))
        for tap in range(taps)
    ]
    gains = jnp.stack([grad_gain, grad_gain_two]).reshape(2, at.ny, half).swapaxes(0, 1)
    gain_sum = take(gains, at.y)
    for j in range(1, at.ny):
        gain_sum = gain_sum + at.shift(take(gains, (at.y - j) % at.ny), dy=-j)
    sums = jnp.concatenate(
        [jnp.stack(conv_sums + [jnp.sum(d_conv, axis=0), grad_bias_a, grad_bias_x, grad_lru]), gain_sum]
    )
    sums = sums.reshape(nvec, *shards, shard).transpose(1, 2, 3, 0, 4)
    sums = scatter_shards(at, sums, F32)
    return (
        outputs,
        input_grad,
        sums[taps + 4],
        grad_branch,
        grad_input,
        sums[:taps],
        sums[taps],
        grad_gate_a,
        sums[taps + 1],
        grad_gate_x,
        sums[taps + 2],
        sums[taps + 3],
        grad_w_out,
        sums[taps + 5],
        grad_w_gate_up,
        grad_w_down,
    )


def solution(mesh):
    rows = P(("fsdp", "seq"), None)
    vector = P(("fsdp", "seq"))
    tokens = P("fsdp", "seq", None)
    taps = P(None, ("fsdp", "seq"))
    columns = P(None, None, ("fsdp", "seq"))
    in_specs = (
        tokens, tokens, vector, rows, rows, taps, vector, rows,
        vector, rows, vector, vector, rows, vector, columns, rows,
    )
    out_specs = (
        tokens, tokens, vector, rows, rows, taps, vector, rows,
        vector, rows, vector, vector, rows, vector, columns, rows,
    )
    return jax.shard_map(body, mesh=mesh, in_specs=in_specs, out_specs=out_specs, check_vma=False)
```
